64 devices in a mesh: rep: 4 (over x, y), dp: 16 (over z, core).
Axes of the slice: x: 2, y: 2, z: 8, core: 2. Of those that a mesh axis runs over, the one named last changes fastest.
The devices are a block of a 4x4x8 slice.
Arguments:
- g_w_gate: bfloat16 [64, 2, 640, 3456], P(('rep', 'dp')), parts along dimension 0
- g_w_up: bfloat16 [64, 2, 640, 3456], P(('rep', 'dp')), parts along dimension 0
- g_w_down: bfloat16 [64, 2, 3456, 640], P(('rep', 'dp')), parts along dimension 0
- w_gate: bfloat16 [2, 640, 3456], replicated
- w_up: bfloat16 [2, 640, 3456], replicated
- w_down: bfloat16 [2, 3456, 640], replicated
- m_w_gate: float32 [2, 640, 3456], P(None, 'dp')
- m_w_up: float32 [2, 640, 3456], P(None, 'dp')
- m_w_down: float32 [2, 3456, 640], P(None, 'dp')
- v_w_gate: float32 [2, 640, 3456], P(None, 'dp')
- v_w_up: float32 [2, 640, 3456], P(None, 'dp')
- v_w_down: float32 [2, 3456, 640], P(None, 'dp')
Outputs:
- output 1: bfloat16 [8, 640, 3456], P('rep'), parts along dimension 0
- output 2: bfloat16 [8, 640, 3456], P('rep'), parts along dimension 0
- output 3: bfloat16 [8, 3456, 640], P('rep'), parts along dimension 0
- output 4: float32 [8, 640, 3456], P('rep', 'dp'), parts along dimension 0
- output 5: float32 [8, 640, 3456], P('rep', 'dp'), parts along dimension 0
- output 6: float32 [8, 3456, 640], P('rep', 'dp'), parts along dimension 0
- output 7: float32 [8, 640, 3456], P('rep', 'dp'), parts along dimension 0
- output 8: float32 [8, 640, 3456], P('rep', 'dp'), parts along dimension 0
- output 9: float32 [8, 3456, 640], P('rep', 'dp'), parts along dimension 0
There are 4 independent parts. The reference program is written for one: setup_inputs(seed, part) draws one part's arguments, and reference() takes and returns one part's arrays. A program takes and returns all parts, laid end to end along the dimension named above; an argument that names none is the same for every part.
All inputs are finite; a program needn't handle non-finite values.
Results may differ from the reference program's by a relative error of at most 0.022.
Values are sent between devices in bfloat16 or wider.
A program may use at most 768 MiB of HBM per device.

```python
import jax
import jax.numpy as jnp
from jax import lax

DEVICES = 16
D = 640
FF = 3456
LAYERS = 2
NAMES = ("w_gate", "w_up", "w_down")
SHAPES = {"w_gate": (LAYERS, D, FF), "w_up": (LAYERS, D, FF), "w_down": (LAYERS, FF, D)}


def setup_inputs(seed: int = 0, part: int = 0) -> dict:
    kz, *keys = jax.random.split(jax.random.key(seed), 1 + 5 * len(NAMES))
    loud = 2.0 ** jax.random.uniform(kz, (), jnp.float32, -1.0, 1.0)
    drawn = {}
    for name, key, both in zip(NAMES, keys[:3], keys[3:6], strict=True):
        own = jax.random.normal(jax.random.fold_in(key, part), (DEVICES, *SHAPES[name]), jnp.float32)
        shared = jax.random.normal(jax.random.fold_in(both, part), SHAPES[name], jnp.float32)
        drawn["g_" + name] = (loud * (0.7 * shared / DEVICES + 0.7 * own * DEVICES**-0.5)).astype(jnp.bfloat16)
    for name, key in zip(NAMES, keys[6:9], strict=True):
        drawn[name] = (jax.random.normal(key, SHAPES[name], jnp.float32) * SHAPES[name][1] ** -0.5).astype(jnp.bfloat16)
    for name, key in zip(NAMES, keys[9:12], strict=True):
        drawn["m_" + name] = loud * 0.5 * jax.random.normal(key, SHAPES[name], jnp.float32)
    for name, key in zip(NAMES, keys[12:15], strict=True):
        drawn["v_" + name] = loud * loud * jax.random.uniform(key, SHAPES[name], jnp.float32, 0.5, 1.5)
    return drawn


def adamw(w, m, v, g):
    m = 0.9 * m + 0.1 * g
    v = 0.95 * v + 0.05 * g * g
    step = m * lax.rsqrt(v + 1e-8) + 0.1 * w
    return (w - 0.02 * step).astype(jnp.bfloat16), m, v


def reference(g_w_gate, g_w_up, g_w_down, w_gate, w_up, w_down, m_w_gate, m_w_up, m_w_down, v_w_gate, v_w_up, v_w_down):
    def total(terms):
        return lax.scan(lambda so_far, term: (so_far + term.astype(jnp.float32), None), jnp.zeros(terms.shape[1:], jnp.float32), terms)[0]

    gradients = [total(terms).astype(jnp.bfloat16).astype(jnp.float32) for terms in (g_w_gate, g_w_up, g_w_down)]
    new = [
        adamw(w.astype(jnp.float32), m, v, g)
        for w, m, v, g in zip((w_gate, w_up, w_down), (m_w_gate, m_w_up, m_w_down), (v_w_gate, v_w_up, v_w_down), gradients, strict=True)
    ]
    return tuple(one[which] for which in range(3) for one in new)
```

```python
import functools

import jax
import jax.numpy as jnp
from jax import lax
from jax.experimental import pallas as pl
from jax.experimental.pallas import tpu as pltpu
from jax.sharding import PartitionSpec as P

MESH = pl.DeviceIdType.MESH
F32 = jnp.float32
BF16 = jnp.bfloat16
TILE = 8


def adamw(w, m, v, g):
    m = 0.9 * m + 0.1 * g
    v = 0.95 * v + 0.05 * g * g
    step = m * lax.rsqrt(v + 1e-8) + 0.1 * w
    return (w - 0.02 * step).astype(BF16), m, v


def rows_loop(rows, cols, body):
    step = TILE
    while rows % (2 * step) == 0 and 2 * step * cols <= 32 * 1024:
        step *= 2
    while rows % (3 * step) == 0 and 3 * step * cols <= 32 * 1024:
        step *= 3

    def one(i, carry):
        body(pl.ds(pl.multiple_of(i * step, TILE), step))
        return carry

    lax.fori_loop(0, rows // step, one, 0)


def kernel(n, *refs):
    g, w, m_in, v_in, w_out, m_out, v_out = (refs[i : i + 3] for i in range(0, 21, 3))
    own, term, run = (refs[i : i + 3] for i in range(21, 30, 3))
    own_sem, mom_sem, term_send, term_recv, rs_send, rs_recv, ag_send, ag_recv, fw_send, fw_recv = refs[30:]
    chips = n // 2
    me = lax.axis_index("dp")
    z, core = me // 2, lax.rem(me, 2)
    partner = me + 1 - 2 * core
    sign = (1, -1)
    ahead = [lax.rem(me + 2 * sign[d] + n, n) for d in range(2)]
    chunks = [(k, d) for k in range(3) for d in range(2)]

    def rs_block(d, s):
        return lax.rem(z - sign[d] * (s + 1) + 2 * chips, chips)

    def ag_block(d, t):
        return lax.rem(z - sign[d] * t + chips, chips)

    def own_copy(k, d, s):
        return pltpu.make_async_copy(g[k].at[d, 2 * rs_block(d, s) + core], own[k].at[d, lax.rem(s, 2)], own_sem.at[d, lax.rem(s, 2), k])

    def remote(src, dst, send, recv, to):
        return pltpu.make_async_remote_copy(src_ref=src, dst_ref=dst, send_sem=send, recv_sem=recv, device_id={"dp": to}, device_id_type=MESH)

    def term_copy(k, d, s):
        src = g[k].at[d, 2 * rs_block(d, s) + 1 - core]
        return remote(src, term[k].at[d, s], term_send.at[d, lax.rem(s, 2), k], term_recv.at[d, s, k], partner)

    def rs_copy(k, d, s):
        return remote(term[k].at[d, s], run[k].at[d, s], rs_send.at[d, lax.rem(s, 2), k], rs_recv.at[d, s, k], ahead[d])

    def ag_copy(k, d, t):
        at = w_out[k].at[d, 2 * ag_block(d, t) + core]
        return remote(at, at, ag_send.at[d, lax.rem(t, 2), k], ag_recv.at[d, t, k], ahead[d])

    def ag_arrival(k, d, t):
        at = w_out[k].at[d, 2 * ag_block(d, t + 1) + core]
        return remote(at, at, ag_send.at[d, lax.rem(t, 2), k], ag_recv.at[d, t, k], ahead[d])

    def fw_copy(k, d, t, whose):
        at = w_out[k].at[d, 2 * ag_block(d, t) + whose]
        return remote(at, at, fw_send.at[d, lax.rem(t, 2), k], fw_recv.at[d, t, k], partner)

    def mom_copies(k, d):
        return (
            pltpu.make_async_copy(m_in[k].at[d], m_out[k].at[d], mom_sem.at[0, d, k]),
            pltpu.make_async_copy(v_in[k].at[d], v_out[k].at[d], mom_sem.at[1, d, k]),
            pltpu.make_async_copy(w[k].at[d, me], w_out[k].at[d, me], mom_sem.at[2, d, k]),
        )

    for k, d in chunks:
        own_copy(k, d, 0).start()

    barrier = pltpu.get_barrier_semaphore()
    for peer in (partner, *ahead):
        pl.semaphore_signal(barrier, inc=1, device_id={"dp": peer}, device_id_type=MESH)
    pl.semaphore_wait(barrier, 3)

    for k, d in chunks:
        term_copy(k, d, 0).start()

    def scatter_step(s, first):
        for k, d in chunks:
            own_copy(k, d, s).wait()
            term_copy(k, d, s).wait_recv()
            if not first:
                rs_copy(k, d, s - 1).wait_recv()
            mine, other, sums = own[k].at[d, lax.rem(s, 2)], term[k].at[d, s], run[k].at[d, s - 1]

            def add(at):
                total = mine[at, :].astype(F32) + other[at, :].astype(F32)
                if not first:
                    total += sums[at, :].astype(F32)
                other[at, :] = total.astype(BF16)

            rows_loop(mine.shape[0], mine.shape[1], add)
            own_copy(k, d, s + 1).start()
            if not first:
                term_copy(k, d, s - 1).wait_send()
            term_copy(k, d, s + 1).start()
            if first:
                for copy in mom_copies(k, d):
                    copy.start()
            if not first:

                @pl.when(s >= 2)
                def _():
                    rs_copy(k, d, s - 2).wait_send()

            rs_copy(k, d, s).start()

    scatter_step(0, True)
    lax.fori_loop(1, chips - 1, lambda s, c: (scatter_step(s, False), c)[1], 0)

    last = chips - 1
    for k, d in chunks:
        own_copy(k, d, last).wait()
        term_copy(k, d, last).wait_recv()
        rs_copy(k, d, last - 1).wait_recv()
        for copy in mom_copies(k, d):
            copy.wait()
        mine, other, sums = own[k].at[d, last % 2], term[k].at[d, last], run[k].at[d, last - 1]
        mo, vo, wo = m_out[k].at[d], v_out[k].at[d], w_out[k].at[d, me]

        def update(at):
            total = mine[at, :].astype(F32) + other[at, :].astype(F32) + sums[at, :].astype(F32)
            grad = total.astype(BF16).astype(F32)
            new_w, new_m, new_v = adamw(wo[at, :].astype(F32), mo[at, :], vo[at, :], grad)
            mo[at, :] = new_m
            vo[at, :] = new_v
            wo[at, :] = new_w

        rows_loop(mine.shape[0], mine.shape[1], update)
        term_copy(k, d, last - 1).wait_send()
        term_copy(k, d, last).wait_send()
        ag_copy(k, d, 0).start()
        fw_copy(k, d, 0, core).start()
        rs_copy(k, d, last - 2).wait_send()

    def gather_step(t, c):
        for k, d in chunks:
            ag_arrival(k, d, t - 1).wait_recv()

            @pl.when(t >= 2)
            def _():
                ag_copy(k, d, t - 2).wait_send()
                fw_copy(k, d, t - 2, core).wait_send()

            ag_copy(k, d, t).start()
            fw_copy(k, d, t, core).start()
        return c

    lax.fori_loop(1, chips - 1, gather_step, 0)
    for k, d in chunks:
        ag_arrival(k, d, last - 1).wait_recv()
        fw_copy(k, d, last - 2, core).wait_send()
        fw_copy(k, d, last, core).start()
    for k, d in chunks:
        rs_copy(k, d, last - 1).wait_send()
        ag_copy(k, d, last - 2).wait_send()
        ag_copy(k, d, last - 1).wait_send()
        fw_copy(k, d, last - 1, core).wait_send()
        fw_copy(k, d, last, core).wait_send()

    def landed(t, c):
        for k, d in chunks:
            fw_copy(k, d, t, 1 - core).wait_recv()
        return c

    lax.fori_loop(0, chips, landed, 0)


def write_out(*refs):
    count = len(refs) // 2
    copies = []
    for i in range(count):
        for j in range(refs[i].shape[0]):
            copies.append(pltpu.make_async_copy(refs[i].at[j], refs[count + i].at[j], refs[-1].at[i, j]))
    for copy in copies:
        copy.start()
    for copy in copies:
        copy.wait()


def solution(mesh):
    n = mesh.shape["dp"]
    chips = n // 2

    def step(*arrays):
        terms, weights, m, v = (arrays[i : i + 3] for i in (0, 3, 6, 9))
        layers = m[0].shape[0]
        blocks = [(one.shape[1], one.shape[2]) for one in m]
        terms = [t.reshape(layers, n, *b) for t, b in zip(terms, blocks, strict=True)]
        weights = [w.reshape(layers, n, *b) for w, b in zip(weights, blocks, strict=True)]
        dma = pltpu.SemaphoreType.DMA
        out = pl.pallas_call(
            functools.partial(kernel, n),
            out_shape=[pltpu.VMEM((layers, n, *b), BF16) for b in blocks] + [pltpu.VMEM((layers, *b), F32) for b in blocks] * 2,
            in_specs=[pl.BlockSpec(memory_space=pltpu.HBM)] * 12,
            out_specs=[pl.BlockSpec(memory_space=pltpu.VMEM)] * 9,
            scratch_shapes=[
                *(pltpu.VMEM((layers, 2, *b), BF16) for b in blocks),
                *(pltpu.VMEM((layers, chips, *b), BF16) for b in blocks),
                *(pltpu.VMEM((layers, chips - 1, *b), BF16) for b in blocks),
                dma((layers, 2, 3)),
                dma((3, layers, 3)),
                dma((layers, 2, 3)),
                dma((layers, chips, 3)),
                dma((layers, 2, 3)),
                dma((layers, chips - 1, 3)),
                dma((layers, 2, 3)),
                dma((layers, chips - 1, 3)),
                dma((layers, 2, 3)),
                dma((layers, chips, 3)),
            ],
            compiler_params=pltpu.CompilerParams(collective_id=0, has_side_effects=True, vmem_limit_bytes=28 * 1024 * 1024),
        )(*terms, *weights, *m, *v)
        out = [pl.pallas_call(
            write_out,
            out_shape=[pltpu.HBM(o.shape, o.dtype) for o in part],
            in_specs=[pl.BlockSpec(memory_space=pltpu.VMEM)] * len(part),
            out_specs=[pl.BlockSpec(memory_space=pltpu.HBM)] * len(part),
            scratch_shapes=[dma((9, layers))],
            compiler_params=pltpu.CompilerParams(vmem_limit_bytes=1024 * 1024),
        )(*part) for part in (out[:3], out[3:])]
        out = [x for p in out for x in p]
        whole = [one.reshape(layers, n * b[0], b[1]) for one, b in zip(out[:3], blocks, strict=True)]
        return (*whole, *out[3:])

    all_of, cut = P(None, None, None), P(None, "dp", None)
    return jax.shard_map(
        step,
        mesh=mesh,
        in_specs=(P(("rep", "dp"), None, None, None),) * 3 + (all_of,) * 3 + (cut,) * 6,
        out_specs=(P("rep", None, None),) * 3 + (P("rep", "dp", None),) * 6,
        check_vma=False,
    )
```

```python
import functools

import jax
import jax.numpy as jnp
from jax import lax
from jax.experimental import pallas as pl
from jax.experimental.pallas import tpu as pltpu
from jax.sharding import PartitionSpec as P

MESH = pl.DeviceIdType.MESH
F32 = jnp.float32
BF16 = jnp.bfloat16
TILE = 8


def adamw(w, m, v, g):
    m = 0.9 * m + 0.1 * g
    v = 0.95 * v + 0.05 * g * g
    step = m * lax.rsqrt(v + 1e-8) + 0.1 * w
    return (w - 0.02 * step).astype(BF16), m, v


def units_of(blocks):
    units = []
    for k, (rows, cols) in enumerate(blocks):
        short = TILE * max(1, 8 * 3456 // (TILE * cols))
        if k == 0:
            units += [(k, 0, short), (k, short, rows - short)]
        elif k == len(blocks) - 1:
            units += [(k, 0, rows - short), (k, rows - short, short)]
        else:
            units.append((k, 0, rows))
    return units


def rows_loop(first, rows, cols, body):
    step = TILE
    while rows % (2 * step) == 0 and 2 * step * cols <= 32 * 1024:
        step *= 2
    while rows % (3 * step) == 0 and 3 * step * cols <= 32 * 1024:
        step *= 3

    def one(i, carry):
        body(pl.ds(pl.multiple_of(first + i * step, TILE), step))
        return carry

    lax.fori_loop(0, rows // step, one, 0)


def kernel(n, *refs):
    g, w, m_in, v_in, w_out, m_out, v_out = (refs[i : i + 3] for i in range(0, 21, 3))
    own, term, run = (refs[i : i + 3] for i in range(21, 30, 3))
    own_sem, mom_sem, term_send, term_recv, rs_send, rs_recv, ag_send, ag_recv, fw_send, fw_recv = refs[30:]
    chips = n // 2
    me = lax.axis_index("dp")
    z, core = me // 2, lax.rem(me, 2)
    partner = me + 1 - 2 * core
    sign = (1, -1)
    ahead = [lax.rem(me + 2 * sign[d] + n, n) for d in range(2)]
    units = units_of([one.shape[1:] for one in m_in])
    chunks = [(u, d) for u in range(len(units)) for d in range(2)]

    def part(refs, u, *at):
        k, first, rows = units[u]
        return refs[k].at[(*at, pl.ds(first, rows))]

    def rs_block(d, s):
        return lax.rem(z - sign[d] * (s + 1) + 2 * chips, chips)

    def ag_block(d, t):
        return lax.rem(z - sign[d] * t + chips, chips)

    def own_copy(u, d, s):
        at = lax.rem(s, 2)
        return pltpu.make_async_copy(part(g, u, d, 2 * rs_block(d, s) + core), part(own, u, d, at), own_sem.at[d, at, u])

    def remote(src, dst, send, recv, to):
        return pltpu.make_async_remote_copy(src_ref=src, dst_ref=dst, send_sem=send, recv_sem=recv, device_id={"dp": to}, device_id_type=MESH)

    def term_copy(u, d, s):
        src = part(g, u, d, 2 * rs_block(d, s) + 1 - core)
        return remote(src, part(term, u, d, s), term_send.at[d, lax.rem(s, 2), u], term_recv.at[d, s, u], partner)

    def rs_copy(u, d, s):
        return remote(part(term, u, d, s), part(run, u, d, s), rs_send.at[d, lax.rem(s, 2), u], rs_recv.at[d, s, u], ahead[d])

    def ag_copy(u, d, t, block=None):
        at = part(w_out, u, d, 2 * (ag_block(d, t) if block is None else block) + core)
        return remote(at, at, ag_send.at[d, lax.rem(t, 2), u], ag_recv.at[d, t, u], ahead[d])

    def ag_arrival(u, d, t):
        return ag_copy(u, d, t, ag_block(d, t + 1))

    def fw_copy(u, d, t, whose):
        at = part(w_out, u, d, 2 * ag_block(d, t) + whose)
        return remote(at, at, fw_send.at[d, lax.rem(t, 2), u], fw_recv.at[d, t, u], partner)

    def mom_copies(u, d):
        return (
            pltpu.make_async_copy(part(m_in, u, d), part(m_out, u, d), mom_sem.at[0, d, u]),
            pltpu.make_async_copy(part(v_in, u, d), part(v_out, u, d), mom_sem.at[1, d, u]),
            pltpu.make_async_copy(part(w, u, d, me), part(w_out, u, d, me), mom_sem.at[2, d, u]),
        )

    for u, d in chunks:
        own_copy(u, d, 0).start()

    barrier = pltpu.get_barrier_semaphore()
    for peer in (partner, *ahead):
        pl.semaphore_signal(barrier, inc=1, device_id={"dp": peer}, device_id_type=MESH)
    pl.semaphore_wait(barrier, 3)

    for u, d in chunks:
        term_copy(u, d, 0).start()

    def scatter_step(s, first):
        for u, d in chunks:
            k, row, rows = units[u]
            own_copy(u, d, s).wait()
            term_copy(u, d, s).wait_recv()
            if not first:
                rs_copy(u, d, s - 1).wait_recv()
            mine, other, sums = own[k].at[d, lax.rem(s, 2)], term[k].at[d, s], run[k].at[d, s - 1]

            def add(at):
                total = mine[at, :].astype(F32) + other[at, :].astype(F32)
                if not first:
                    total += sums[at, :].astype(F32)
                other[at, :] = total.astype(BF16)

            rows_loop(row, rows, mine.shape[1], add)
            own_copy(u, d, s + 1).start()
            if not first:
                term_copy(u, d, s - 1).wait_send()
            term_copy(u, d, s + 1).start()
            if not first:

                @pl.when(s >= 2)
                def _():
                    rs_copy(u, d, s - 2).wait_send()

            rs_copy(u, d, s).start()
            if first:
                for copy in mom_copies(u, d):
                    copy.start()

    scatter_step(0, True)
    lax.fori_loop(1, chips - 1, lambda s, c: (scatter_step(s, False), c)[1], 0)

    last = chips - 1
    for u, d in chunks:
        k, row, rows = units[u]
        own_copy(u, d, last).wait()
        term_copy(u, d, last).wait_recv()
        for copy in mom_copies(u, d):
            copy.wait()
        rs_copy(u, d, last - 1).wait_recv()
        mine, other, sums = own[k].at[d, last % 2], term[k].at[d, last], run[k].at[d, last - 1]
        mo, vo, wo = m_out[k].at[d], v_out[k].at[d], w_out[k].at[d, me]

        def update(at):
            total = mine[at, :].astype(F32) + other[at, :].astype(F32) + sums[at, :].astype(F32)
            grad = total.astype(BF16).astype(F32)
            new_w, new_m, new_v = adamw(wo[at, :].astype(F32), mo[at, :], vo[at, :], grad)
            mo[at, :] = new_m
            vo[at, :] = new_v
            wo[at, :] = new_w

        rows_loop(row, rows, mine.shape[1], update)
        term_copy(u, d, last - 1).wait_send()
        term_copy(u, d, last).wait_send()
        ag_copy(u, d, 0).start()
        fw_copy(u, d, 0, core).start()
        rs_copy(u, d, last - 2).wait_send()

    def gather_step(t, c):
        for u, d in chunks:
            ag_arrival(u, d, t - 1).wait_recv()

            @pl.when(t >= 2)
            def _():
                ag_copy(u, d, t - 2).wait_send()
                fw_copy(u, d, t - 2, core).wait_send()

            ag_copy(u, d, t).start()
            fw_copy(u, d, t, core).start()
        return c

    lax.fori_loop(1, chips - 1, gather_step, 0)
    for u, d in chunks:
        ag_arrival(u, d, last - 1).wait_recv()
        fw_copy(u, d, last - 2, core).wait_send()
        fw_copy(u, d, last, core).start()
    for u, d in chunks:
        rs_copy(u, d, last - 1).wait_send()
        ag_copy(u, d, last - 2).wait_send()
        ag_copy(u, d, last - 1).wait_send()
        fw_copy(u, d, last - 1, core).wait_send()
        fw_copy(u, d, last, core).wait_send()

    def landed(t, c):
        for u, d in chunks:
            fw_copy(u, d, t, 1 - core).wait_recv()
        return c

    lax.fori_loop(0, chips, landed, 0)


def write_out(*refs):
    count = len(refs) // 2
    copies = []
    for i in range(count):
        for j in range(refs[i].shape[0]):
            copies.append(pltpu.make_async_copy(refs[i].at[j], refs[count + i].at[j], refs[-1].at[i, j]))
    for copy in copies:
        copy.start()
    for copy in copies:
        copy.wait()


def solution(mesh):
    n = mesh.shape["dp"]
    chips = n // 2

    def step(*arrays):
        terms, weights, m, v = (arrays[i : i + 3] for i in (0, 3, 6, 9))
        layers = m[0].shape[0]
        blocks = [(one.shape[1], one.shape[2]) for one in m]
        terms = [t.reshape(layers, n, *b) for t, b in zip(terms, blocks, strict=True)]
        weights = [w.reshape(layers, n, *b) for w, b in zip(weights, blocks, strict=True)]
        dma = pltpu.SemaphoreType.DMA
        count = len(units_of(blocks))
        out = pl.pallas_call(
            functools.partial(kernel, n),
            out_shape=[pltpu.VMEM((layers, n, *b), BF16) for b in blocks] + [pltpu.VMEM((layers, *b), F32) for b in blocks] * 2,
            in_specs=[pl.BlockSpec(memory_space=pltpu.HBM)] * 12,
            out_specs=[pl.BlockSpec(memory_space=pltpu.VMEM)] * 9,
            scratch_shapes=[
                *(pltpu.VMEM((layers, 2, *b), BF16) for b in blocks),
                *(pltpu.VMEM((layers, chips, *b), BF16) for b in blocks),
                *(pltpu.VMEM((layers, chips - 1, *b), BF16) for b in blocks),
                dma((layers, 2, count)),
                dma((3, layers, count)),
                dma((layers, 2, count)),
                dma((layers, chips, count)),
                dma((layers, 2, count)),
                dma((layers, chips - 1, count)),
                dma((layers, 2, count)),
                dma((layers, chips - 1, count)),
                dma((layers, 2, count)),
                dma((layers, chips, count)),
            ],
            compiler_params=pltpu.CompilerParams(collective_id=0, has_side_effects=True, vmem_limit_bytes=28 * 1024 * 1024),
        )(*terms, *weights, *m, *v)
        out = [pl.pallas_call(
            write_out,
            out_shape=[pltpu.HBM(o.shape, o.dtype) for o in part],
            in_specs=[pl.BlockSpec(memory_space=pltpu.VMEM)] * len(part),
            out_specs=[pl.BlockSpec(memory_space=pltpu.HBM)] * len(part),
            scratch_shapes=[dma((9, layers))],
            compiler_params=pltpu.CompilerParams(vmem_limit_bytes=1024 * 1024),
        )(*part) for part in (out[:3], out[3:])]
        out = [x for p in out for x in p]
        whole = [one.reshape(layers, n * b[0], b[1]) for one, b in zip(out[:3], blocks, strict=True)]
        return (*whole, *out[3:])

    all_of, cut = P(None, None, None), P(None, "dp", None)
    return jax.shard_map(
        step,
        mesh=mesh,
        in_specs=(P(("rep", "dp"), None, None, None),) * 3 + (all_of,) * 3 + (cut,) * 6,
        out_specs=(P("rep", None, None),) * 3 + (P("rep", "dp", None),) * 6,
        check_vma=False,
    )
```

```python
import functools

import jax
import jax.numpy as jnp
from jax import lax
from jax.experimental import pallas as pl
from jax.experimental.pallas import tpu as pltpu
from jax.sharding import PartitionSpec as P

MESH = pl.DeviceIdType.MESH
F32 = jnp.float32
BF16 = jnp.bfloat16
TILE = 8


def adamw(w, m, v, g):
    m = 0.9 * m + 0.1 * g
    v = 0.95 * v + 0.05 * g * g
    step = m * lax.rsqrt(v + 1e-8) + 0.1 * w
    return (w - 0.02 * step).astype(BF16), m, v


def units_of(blocks):
    units = []
    for k, (rows, cols) in enumerate(blocks):
        if k == 0:
            units += [(k, 0, TILE), (k, TILE, rows - TILE)]
        else:
            units.append((k, 0, rows))
    return units


def rows_loop(first, rows, cols, body):
    step = TILE
    while rows % (2 * step) == 0 and 2 * step * cols <= 32 * 1024:
        step *= 2
    while rows % (3 * step) == 0 and 3 * step * cols <= 32 * 1024:
        step *= 3

    def one(i, carry):
        body(pl.ds(pl.multiple_of(first + i * step, TILE), step))
        return carry

    lax.fori_loop(0, rows // step, one, 0)


def kernel(n, *refs):
    g, w, m_in, v_in, w_out, m_out, v_out = (refs[i : i + 3] for i in range(0, 21, 3))
    own, term, run = (refs[i : i + 3] for i in range(21, 30, 3))
    own_sem, mom_sem, term_send, term_recv, rs_send, ag_send, ring_recv, fw_send, fw_recv = refs[30:]
    chips = n // 2
    me = lax.axis_index("dp")
    z, core = me // 2, lax.rem(me, 2)
    partner = me + 1 - 2 * core
    sign = (1, -1)
    ahead = [lax.rem(me + 2 * sign[d] + n, n) for d in range(2)]
    units = units_of([one.shape[1:] for one in m_in])
    chunks = [(u, d) for u in range(len(units)) for d in range(2)]

    def part(refs, u, *at):
        k, first, rows = units[u]
        return refs[k].at[(*at, pl.ds(first, rows))]

    def rs_block(d, s):
        return lax.rem(z - sign[d] * (s + 1) + 2 * chips, chips)

    def ag_block(d, t):
        return lax.rem(z - sign[d] * t + chips, chips)

    def own_copy(u, d, s):
        at = lax.rem(s, 2)
        return pltpu.make_async_copy(part(g, u, d, 2 * rs_block(d, s) + core), part(own, u, d, at), own_sem.at[d, at, u])

    def remote(src, dst, send, recv, to):
        return pltpu.make_async_remote_copy(src_ref=src, dst_ref=dst, send_sem=send, recv_sem=recv, device_id={"dp": to}, device_id_type=MESH)

    def term_copy(u, d, s):
        src = part(g, u, d, 2 * rs_block(d, s) + 1 - core)
        return remote(src, part(term, u, d, s), term_send.at[units[u][0]], term_recv.at[d, lax.rem(s, 2), u], partner)

    def rs_copy(u, d, s):
        return remote(part(term, u, d, s), part(run, u, d, s), rs_send.at[units[u][0]], ring_recv.at[d, s, u], ahead[d])

    def ag_copy(u, d, t, block=None):
        at = part(w_out, u, d, 2 * (ag_block(d, t) if block is None else block) + core)
        return remote(at, at, ag_send.at[units[u][0]], ring_recv.at[d, lax.rem(chips - 1 + t, chips), u], ahead[d])

    def ag_arrival(u, d, t):
        return ag_copy(u, d, t, ag_block(d, t + 1))

    def fw_copy(u, d, t, whose):
        at = part(w_out, u, d, 2 * ag_block(d, t) + whose)
        return remote(at, at, fw_send.at[units[u][0]], fw_recv.at[units[u][0]], partner)

    def mom_copies(k):
        return (
            pltpu.make_async_copy(m_in[k], m_out[k], mom_sem.at[0, k]),
            pltpu.make_async_copy(v_in[k], v_out[k], mom_sem.at[1, k]),
            pltpu.make_async_copy(w[k].at[:, me], w_out[k].at[:, me], mom_sem.at[2, k]),
        )

    def all_of(k, blocks, send, recv):
        at = w_out[k].at[0, pl.ds(0, blocks)]
        return remote(at, at, send.at[k], recv.at[k], partner)

    for u, d in chunks:
        own_copy(u, d, 0).start()

    barrier = pltpu.get_barrier_semaphore()
    for peer in (partner, *ahead):
        pl.semaphore_signal(barrier, inc=1, device_id={"dp": peer}, device_id_type=MESH)
    pl.semaphore_wait(barrier, 3)

    for u, d in chunks:
        term_copy(u, d, 0).start()

    def scatter_step(s, first):
        for u, d in chunks:
            k, row, rows = units[u]
            own_copy(u, d, s).wait()
            term_copy(u, d, s).wait_recv()
            if not first:
                rs_copy(u, d, s - 1).wait_recv()
            mine, other, sums = own[k].at[d, lax.rem(s, 2)], term[k].at[d, s], run[k].at[d, s - 1]

            def add(at):
                total = mine[at, :].astype(F32) + other[at, :].astype(F32)
                if not first:
                    total += sums[at, :].astype(F32)
                other[at, :] = total.astype(BF16)

            rows_loop(row, rows, mine.shape[1], add)
            own_copy(u, d, s + 1).start()
            rs_copy(u, d, s).start()
            term_copy(u, d, s + 1).start()

    scatter_step(0, True)
    for k in range(3):
        for copy in mom_copies(k):
            copy.start()
    lax.fori_loop(1, chips - 1, lambda s, c: (scatter_step(s, False), c)[1], 0)

    last = chips - 1
    for u, d in chunks:
        k, row, rows = units[u]
        own_copy(u, d, last).wait()
        term_copy(u, d, last).wait_recv()
        if d == 0 and row == 0:
            for copy in mom_copies(k):
                copy.wait()
        rs_copy(u, d, last - 1).wait_recv()
        mine, other, sums = own[k].at[d, last % 2], term[k].at[d, last], run[k].at[d, last - 1]
        mo, vo, wo = m_out[k].at[d], v_out[k].at[d], w_out[k].at[d, me]

        def update(at):
            total = mine[at, :].astype(F32) + other[at, :].astype(F32) + sums[at, :].astype(F32)
            grad = total.astype(BF16).astype(F32)
            new_w, new_m, new_v = adamw(wo[at, :].astype(F32), mo[at, :], vo[at, :], grad)
            mo[at, :] = new_m
            vo[at, :] = new_v
            wo[at, :] = new_w

        rows_loop(row, rows, mine.shape[1], update)
        ag_copy(u, d, 0).start()
        fw_copy(u, d, 0, core).start()

    def gather_step(t, c):
        for u, d in chunks:
            ag_arrival(u, d, t - 1).wait_recv()
            ag_copy(u, d, t).start()
            fw_copy(u, d, t, core).start()
        return c

    lax.fori_loop(1, chips - 1, gather_step, 0)
    for u, d in chunks:
        ag_arrival(u, d, last - 1).wait_recv()
        fw_copy(u, d, last, core).start()
    for k in range(3):
        all_of(k, n, term_send, fw_recv).wait_send()
        all_of(k, n - 2, rs_send, fw_recv).wait_send()
        all_of(k, n - 2, ag_send, fw_recv).wait_send()
        all_of(k, n, fw_send, fw_recv).wait()


def write_out(*refs):
    count = len(refs) // 2
    copies = []
    for i in range(count):
        for j in range(refs[i].shape[0]):
            copies.append(pltpu.make_async_copy(refs[i].at[j], refs[count + i].at[j], refs[-1].at[i, j]))
    for copy in copies:
        copy.start()
    for copy in copies:
        copy.wait()


def solution(mesh):
    n = mesh.shape["dp"]
    chips = n // 2

    def step(*arrays):
        terms, weights, m, v = (arrays[i : i + 3] for i in (0, 3, 6, 9))
        layers = m[0].shape[0]
        blocks = [(one.shape[1], one.shape[2]) for one in m]
        terms = [t.reshape(layers, n, *b) for t, b in zip(terms, blocks, strict=True)]
        weights = [w.reshape(layers, n, *b) for w, b in zip(weights, blocks, strict=True)]
        dma = pltpu.SemaphoreType.DMA
        count = len(units_of(blocks))
        out = pl.pallas_call(
            functools.partial(kernel, n),
            out_shape=[pltpu.VMEM((layers, n, *b), BF16) for b in blocks] + [pltpu.VMEM((layers, *b), F32) for b in blocks] * 2,
            in_specs=[pl.BlockSpec(memory_space=pltpu.HBM)] * 12,
            out_specs=[pl.BlockSpec(memory_space=pltpu.VMEM)] * 9,
            scratch_shapes=[
                *(pltpu.VMEM((layers, 2, *b), BF16) for b in blocks),
                *(pltpu.VMEM((layers, chips, *b), BF16) for b in blocks),
                *(pltpu.VMEM((layers, chips - 1, *b), BF16) for b in blocks),
                dma((layers, 2, count)),
                dma((3, 3)),
                dma((3,)),
                dma((layers, 2, count)),
                dma((3,)),
                dma((3,)),
                dma((layers, chips, count)),
                dma((3,)),
                dma((3,)),
            ],
            compiler_params=pltpu.CompilerParams(collective_id=0, has_side_effects=True, vmem_limit_bytes=28 * 1024 * 1024),
        )(*terms, *weights, *m, *v)
        out = [pl.pallas_call(
            write_out,
            out_shape=[pltpu.HBM(o.shape, o.dtype) for o in part],
            in_specs=[pl.BlockSpec(memory_space=pltpu.VMEM)] * len(part),
            out_specs=[pl.BlockSpec(memory_space=pltpu.HBM)] * len(part),
            scratch_shapes=[dma((len(part), layers))],
            compiler_params=pltpu.CompilerParams(vmem_limit_bytes=1024 * 1024),
        )(*part) for part in (out[:3], out[3:])]
        out = [x for p in out for x in p]
        whole = [one.reshape(layers, n * b[0], b[1]) for one, b in zip(out[:3], blocks, strict=True)]
        return (*whole, *out[3:])

    all_of, cut = P(None, None, None), P(None, "dp", None)
    return jax.shard_map(
        step,
        mesh=mesh,
        in_specs=(P(("rep", "dp"), None, None, None),) * 3 + (all_of,) * 3 + (cut,) * 6,
        out_specs=(P("rep", None, None),) * 3 + (P("rep", "dp", None),) * 6,
        check_vma=False,
    )
```

```python
import functools

import jax
import jax.numpy as jnp
from jax import lax
from jax.experimental import pallas as pl
from jax.experimental.pallas import tpu as pltpu
from jax.sharding import PartitionSpec as P

MESH = pl.DeviceIdType.MESH
F32 = jnp.float32
BF16 = jnp.bfloat16
TILE = 8
EARLY = 5
JOIN = 5
CUTS = 7


def adamw(w, m, v, g):
    m = 0.9 * m + 0.1 * g
    v = 0.95 * v + 0.05 * g * g
    step = m * lax.rsqrt(v + 1e-8) + 0.1 * w
    return (w - 0.02 * step).astype(BF16), m, v


def pieces_of(blocks):
    whole = [(k, 0, b[0], k) for k, b in enumerate(blocks)]
    top = blocks[0][0]
    return whole, [(0, 0, TILE, len(blocks)), (0, TILE, top - TILE, 0), *whole[1:]]


def thirds_of(rows):
    tiles = rows // TILE
    count = min(CUTS, tiles)
    cuts = [TILE * (tiles * i // count) for i in range(count + 1)]
    return [(a, b - a) for a, b in zip(cuts, cuts[1:])]


def rows_loop(first, rows, cols, body):
    step = TILE
    while rows % (2 * step) == 0 and 2 * step * cols <= 32 * 1024:
        step *= 2
    while rows % (3 * step) == 0 and 3 * step * cols <= 32 * 1024:
        step *= 3

    def one(i, carry):
        body(pl.ds(pl.multiple_of(first + i * step, TILE), step))
        return carry

    lax.fori_loop(0, rows // step, one, 0)


def kernel(n, *refs):
    g, w, m_in, v_in, w_out, m_out, v_out = (refs[i : i + 3] for i in range(0, 21, 3))
    own, term, run = (refs[i : i + 3] for i in range(21, 30, 3))
    stage, stage_sem, own_sem, own_short, mom_sem, term_recv, term_short, ring_recv, ring_send, chip_send, fw_recv, down_recv, down_send = refs[30:]
    chips = n // 2
    last = chips - 1
    me = lax.axis_index("dp")
    z, core = me // 2, lax.rem(me, 2)
    partner = me + 1 - 2 * core
    sign = (1, -1)
    ahead = [lax.rem(me + 2 * sign[d] + n, n) for d in range(2)]
    whole, head = pieces_of([one.shape[1:] for one in m_in])
    most, thirds = whole[:-1], thirds_of(whole[-1][2])

    def both(pieces):
        return [(p, d) for p in pieces for d in range(2)]

    def part(refs, p, *at):
        return refs[p[0]].at[(*at, pl.ds(p[1], p[2]))]

    def sem(many, short, p, d, slot):
        return short.at[d] if p[3] == len(whole) else many.at[d, slot, p[3]]

    def rs_block(d, s):
        return lax.rem(z - sign[d] * (s + 1) + 2 * chips, chips)

    def ag_block(d, t):
        return lax.rem(z - sign[d] * t + chips, chips)

    def remote(src, dst, send, recv, to):
        return pltpu.make_async_remote_copy(src_ref=src, dst_ref=dst, send_sem=send, recv_sem=recv, device_id={"dp": to}, device_id_type=MESH)

    def own_copy(p, d, s):
        slot = lax.rem(s, 2)
        return pltpu.make_async_copy(part(g, p, d, 2 * rs_block(d, s) + core), part(own, p, d, slot), sem(own_sem, own_short, p, d, slot))

    def stage_copy(p, d):
        return pltpu.make_async_copy(part(g, p, d, 2 * rs_block(d, 0) + 1 - core), stage.at[d], stage_sem.at[d])

    def term_copy(p, d, s, src=None):
        src = part(g, p, d, 2 * rs_block(d, s) + 1 - core) if src is None else src
        return remote(src, part(term, p, d, s), chip_send.at[p[0]], sem(term_recv, term_short, p, d, lax.rem(s, 2)), partner)

    def rs_copy(p, d, s):
        return remote(part(term, p, d, s), part(run, p, d, s), ring_send.at[p[0]], ring_recv.at[d, lax.rem(s, 3), p[0]], ahead[d])

    def ag_copy(p, d, t, block=None):
        at = part(w_out, p, d, 2 * (ag_block(d, t) if block is None else block) + core)
        return remote(at, at, ring_send.at[p[0]], ring_recv.at[d, lax.rem(last + t, 3), p[0]], ahead[d])

    def ag_arrival(p, d, t):
        return ag_copy(p, d, t, ag_block(d, t + 1))

    def fw_copy(p, d, t):
        at = part(w_out, p, d, 2 * ag_block(d, t) + core)
        return remote(at, at, chip_send.at[p[0]], fw_recv.at[p[0]], partner)

    def mom_copies(k):
        return (
            pltpu.make_async_copy(m_in[k], m_out[k], mom_sem.at[k]),
            pltpu.make_async_copy(v_in[k], v_out[k], mom_sem.at[k]),
            pltpu.make_async_copy(w[k].at[:, me], w_out[k].at[:, me], mom_sem.at[k]),
        )

    def bytes_of(at, semaphore):
        return pltpu.make_async_copy(at, at, semaphore)

    barrier = pltpu.get_barrier_semaphore()
    for peer in (partner, *ahead):
        pl.semaphore_signal(barrier, inc=1, device_id={"dp": peer}, device_id_type=MESH)
    for p, d in both(head[:1]):
        stage_copy(p, d).start()
    for p, d in both(head):
        own_copy(p, d, 0).start()
    pl.semaphore_wait(barrier, 3)

    for p, d in both(head):
        if p is head[0]:
            stage_copy(p, d).wait()
            term_copy(p, d, 0, stage.at[d]).start()
        else:
            term_copy(p, d, 0).start()

    def scatter_step(s, pieces, first):
        for p, d in both(pieces):
            k, row, rows, _ = p
            own_copy(p, d, s).wait()
            term_copy(p, d, s).wait_recv()
            if not first:
                rs_copy(p, d, s - 1).wait_recv()
            mine, other, sums = own[k].at[d, lax.rem(s, 2)], term[k].at[d, s], run[k].at[d, s - 1]

            def add(at):
                total = mine[at, :].astype(F32) + other[at, :].astype(F32)
                if not first:
                    total += sums[at, :].astype(F32)
                other[at, :] = total.astype(BF16)

            rows_loop(row, rows, mine.shape[1], add)
            if p[3] < len(whole):
                own_copy(whole[k], d, s + 1).start()
            rs_copy(p, d, s).start()
            if p[3] < len(whole):
                term_copy(whole[k], d, s + 1).start()

    scatter_step(0, head, True)
    for k in range(3):
        for copy in mom_copies(k):
            copy.start()
    lax.fori_loop(1, last, lambda s, c: (scatter_step(s, whole, False), c)[1], 0)

    for p, d in both(whole):
        k, row, rows, _ = p
        own_copy(p, d, last).wait()
        term_copy(p, d, last).wait_recv()
        if d == 0:
            bytes_of(w_out[k].at[0, pl.ds(0, 5 * m_in[k].shape[0])], mom_sem.at[k]).wait()
        rs_copy(p, d, last - 1).wait_recv()
        mine, other, sums = own[k].at[d, last % 2], term[k].at[d, last], run[k].at[d, last - 1]
        mo, vo, wo = m_out[k].at[d], v_out[k].at[d], w_out[k].at[d, me]

        def update(at):
            total = mine[at, :].astype(F32) + other[at, :].astype(F32) + sums[at, :].astype(F32)
            grad = total.astype(BF16).astype(F32)
            new_w, new_m, new_v = adamw(wo[at, :].astype(F32), mo[at, :], vo[at, :], grad)
            wo[at, :] = new_w
            mo[at, :] = new_m
            vo[at, :] = new_v

        rows_loop(row, rows, mine.shape[1], update)
        if p in most:
            ag_copy(p, d, 0).start()
            fw_copy(p, d, 0).start()

    def gather_step(t, c):
        for p, d in both(most):
            ag_arrival(p, d, t - 1).wait_recv()
            ag_copy(p, d, t).start()
            fw_copy(p, d, t).start()
        return c

    lax.fori_loop(1, last, gather_step, 0)
    for p, d in both(most):
        ag_arrival(p, d, last - 1).wait_recv()
        fw_copy(p, d, last).start()

    def down_copy(p, d, t, block):
        at = w_out[-1].at[d, 2 * block + core, pl.ds(p[0], p[1])]
        return remote(at, at, down_send, down_recv.at[d, lax.rem(t, 3), thirds.index(p)], ahead[d])

    @pl.when(core == 1)
    def _():
        for p, d in both(thirds):
            down_copy(p, d, 0, ag_block(d, 0)).start()

        def early_step(t, c):
            for p, d in both(thirds):
                down_copy(p, d, t - 1, ag_block(d, t)).wait_recv()
                down_copy(p, d, t, ag_block(d, t)).start()
            return c

        lax.fori_loop(1, EARLY, early_step, 0)
        for p, d in both(thirds):
            down_copy(p, d, EARLY - 1, ag_block(d, EARLY)).wait_recv()
        bytes_of(w_out[-1].at[0, pl.ds(0, 2 * EARLY)], down_send).wait()

    for k in range(3):
        if k < 2:
            bytes_of(w_out[k].at[:, pl.ds(0, n - 2)], ring_send.at[k]).wait()
            bytes_of(w_out[k], chip_send.at[k]).wait()
            bytes_of(w_out[k].at[0], fw_recv.at[k]).wait()
        else:
            bytes_of(w_out[k].at[0, pl.ds(0, n - 2)], ring_send.at[k]).wait()
            bytes_of(w_out[k].at[0], chip_send.at[k]).wait()


def rest_kernel(n, held, after, rest, ready, ring_send, ring_recv, chip_send, chip_recv):
    chips = n // 2
    last = chips - 1
    me = lax.axis_index("dp")
    z, core = me // 2, lax.rem(me, 2)
    partner = me + 1 - 2 * core
    sign = (1, -1)
    ahead = [lax.rem(me + 2 * sign[d] + n, n) for d in range(2)]
    thirds = thirds_of(held.shape[2])
    pieces = [(p, d) for p in thirds for d in range(2)]
    had = core * EARLY
    join = jnp.where(core == 0, JOIN, EARLY + 1)

    barrier = pltpu.get_barrier_semaphore()
    for peer in ahead:
        pl.semaphore_signal(barrier, inc=1, device_id={"dp": peer}, device_id_type=MESH)

    @pl.when(core == 0)
    def _():
        pl.semaphore_signal(barrier, inc=1, device_id={"dp": partner}, device_id_type=MESH)

    pl.semaphore_wait(barrier, 2 + core)

    @pl.when(core == 1)
    def _():
        pl.semaphore_signal(ready, inc=1, device_id={"dp": partner}, device_id_type=MESH)

    def at(ref, p, d, t):
        return ref.at[d, 2 * lax.rem(z - sign[d] * t + chips, chips) + core, pl.ds(p[0], p[1])]

    def remote(src, dst, send, recv, to):
        return pltpu.make_async_remote_copy(src_ref=src, dst_ref=dst, send_sem=send, recv_sem=recv, device_id={"dp": to}, device_id_type=MESH)

    def ring_copy(src, p, d, t):
        return remote(at(src, p, d, t), at(rest, p, d, t), ring_send, ring_recv.at[d, lax.rem(t, 3), thirds.index(p)], ahead[d])

    def arrive(p, d, t):
        there = at(rest, p, d, t)
        remote(there, there, ring_send, ring_recv.at[d, lax.rem(t - 1, 3), thirds.index(p)], ahead[d]).wait_recv()

    def fw_copy(src, p, d, t):
        return remote(at(src, p, d, t), at(rest, p, d, t), chip_send, chip_recv, partner)

    for p, d in pieces:
        ring_copy(held, p, d, had).start()

    def step(t, c, forward):
        for p, d in pieces:
            arrive(p, d, t)
            ring_copy(rest, p, d, t).start()
            if forward:
                fw_copy(rest, p, d, t).start()
        return c

    def catch_up(src):
        def one(t, c):
            for p, d in pieces:
                fw_copy(src, p, d, t).start()
            return c

        return one

    lax.fori_loop(had + 1, join, functools.partial(step, forward=False), 0)

    @pl.when(core == 0)
    def _():
        pl.semaphore_wait(ready, 1)

    lax.fori_loop(0, had + 1, catch_up(held), 0)
    lax.fori_loop(had + 1, join, catch_up(rest), 0)
    lax.fori_loop(join, last, functools.partial(step, forward=True), 0)
    for p, d in pieces:
        arrive(p, d, last)
        fw_copy(rest, p, d, last).start()

    for which, count in enumerate((2 * last, 2 * (last - EARLY))):

        @pl.when(core == which)
        def _():
            part = rest.at[0, pl.ds(0, count)]
            pltpu.make_async_copy(part, part, ring_send).wait()

    pltpu.make_async_copy(rest.at[0], rest.at[0], chip_send).wait()
    pltpu.make_async_copy(rest.at[0], rest.at[0], chip_recv).wait()


def write_rest(n, held, rest, out, sem):
    chips = n // 2
    me = lax.axis_index("dp")
    z, core = me // 2, lax.rem(me, 2)
    for d, sign in ((0, 1), (1, -1)):
        for t in range(chips):
            block = 2 * lax.rem(z - sign * t + chips, chips) + core
            in_held = t <= core * EARLY
            for src, cond in ((held, in_held), (rest, jnp.logical_not(in_held))):

                @pl.when(cond)
                def _():
                    pltpu.make_async_copy(src.at[d, block], out.at[d, block], sem).start()

            other = 2 * t + 1 - core
            pltpu.make_async_copy(rest.at[d, other], out.at[d, other], sem).start()
    pltpu.make_async_copy(rest, rest, sem).wait()


def write_out(*refs):
    count = len(refs) // 2 - 1
    mark, sem = refs[-2:]
    copies = []
    for i in range(count):
        for j in range(refs[i].shape[0]):
            copies.append(pltpu.make_async_copy(refs[i].at[j], refs[count + i].at[j], sem.at[i, j]))
    for copy in copies:
        copy.start()
    mark[...] = jnp.zeros_like(mark)
    for copy in copies:
        copy.wait()


def solution(mesh):
    n = mesh.shape["dp"]
    chips = n // 2

    def step(*arrays):
        terms, weights, m, v = (arrays[i : i + 3] for i in (0, 3, 6, 9))
        layers = m[0].shape[0]
        blocks = [(one.shape[1], one.shape[2]) for one in m]
        terms = [t.reshape(layers, n, *b) for t, b in zip(terms, blocks, strict=True)]
        weights = [w.reshape(layers, n, *b) for w, b in zip(weights, blocks, strict=True)]
        dma = pltpu.SemaphoreType.DMA
        thirds = thirds_of(blocks[-1][0])
        out = pl.pallas_call(
            functools.partial(kernel, n),
            out_shape=[pltpu.VMEM((layers, n, *b), BF16) for b in blocks] + [pltpu.VMEM((layers, *b), F32) for b in blocks] * 2,
            in_specs=[pl.BlockSpec(memory_space=pltpu.HBM)] * 12,
            out_specs=[pl.BlockSpec(memory_space=pltpu.VMEM)] * 9,
            scratch_shapes=[
                *(pltpu.VMEM((layers, 2, *b), BF16) for b in blocks),
                *(pltpu.VMEM((layers, chips, *b), BF16) for b in blocks),
                *(pltpu.VMEM((layers, chips - 1, *b), BF16) for b in blocks),
                pltpu.VMEM((layers, TILE, blocks[0][1]), BF16),
                dma((layers,)),
                dma((layers, 2, 3)),
                dma((layers,)),
                dma((3,)),
                dma((layers, 2, 3)),
                dma((layers,)),
                dma((layers, 3, 3)),
                dma((3,)),
                dma((3,)),
                dma((3,)),
                dma((layers, 3, len(thirds))),
                dma,
            ],
            compiler_params=pltpu.CompilerParams(collective_id=0, has_side_effects=True, vmem_limit_bytes=28 * 1024 * 1024),
        )(*terms, *weights, *m, *v)
        held, ready = out[2], [*out[:2], *out[3:]]
        *done, mark = pl.pallas_call(
            write_out,
            out_shape=[*(pltpu.HBM(o.shape, o.dtype) for o in ready), jax.ShapeDtypeStruct((TILE, 128), F32)],
            in_specs=[pl.BlockSpec(memory_space=pltpu.VMEM)] * len(ready),
            out_specs=[pl.BlockSpec(memory_space=pltpu.HBM)] * len(ready) + [pl.BlockSpec(memory_space=pltpu.VMEM)],
            scratch_shapes=[dma((len(ready), layers))],
            compiler_params=pltpu.CompilerParams(vmem_limit_bytes=1024 * 1024),
        )(*ready)
        rest = pl.pallas_call(
            functools.partial(rest_kernel, n),
            out_shape=pltpu.VMEM(held.shape, held.dtype),
            in_specs=[pl.BlockSpec(memory_space=pltpu.VMEM)] * 2,
            out_specs=pl.BlockSpec(memory_space=pltpu.VMEM),
            scratch_shapes=[pltpu.SemaphoreType.REGULAR, dma, dma((layers, 3, len(thirds))), dma, dma],
            compiler_params=pltpu.CompilerParams(collective_id=1, has_side_effects=True, vmem_limit_bytes=1024 * 1024),
        )(held, mark)
        down = pl.pallas_call(
            functools.partial(write_rest, n),
            out_shape=pltpu.HBM(held.shape, held.dtype),
            in_specs=[pl.BlockSpec(memory_space=pltpu.VMEM)] * 2,
            out_specs=pl.BlockSpec(memory_space=pltpu.HBM),
            scratch_shapes=[dma],
            compiler_params=pltpu.CompilerParams(vmem_limit_bytes=1024 * 1024),
        )(held, rest)
        out = [*done[:2], down, *done[2:]]
        whole = [one.reshape(layers, n * b[0], b[1]) for one, b in zip(out[:3], blocks, strict=True)]
        return (*whole, *out[3:])

    all_of, cut = P(None, None, None), P(None, "dp", None)
    return jax.shard_map(
        step,
        mesh=mesh,
        in_specs=(P(("rep", "dp"), None, None, None),) * 3 + (all_of,) * 3 + (cut,) * 6,
        out_specs=(P("rep", None, None),) * 3 + (P("rep", "dp", None),) * 6,
        check_vma=False,
    )
```

```python
import functools

import jax
import jax.numpy as jnp
from jax import lax
from jax.experimental import pallas as pl
from jax.experimental.pallas import tpu as pltpu
from jax.sharding import PartitionSpec as P

MESH = pl.DeviceIdType.MESH
F32 = jnp.float32
BF16 = jnp.bfloat16
TILE = 8
EARLY = 6
JOIN = 6
CUTS = 7


def adamw(w, m, v, g):
    m = 0.9 * m + 0.1 * g
    v = 0.95 * v + 0.05 * g * g
    step = m * lax.rsqrt(v + 1e-8) + 0.1 * w
    return (w - 0.02 * step).astype(BF16), m, v


def pieces_of(blocks):
    whole = [(k, 0, b[0], k) for k, b in enumerate(blocks)]
    top = blocks[0][0]
    return whole, [(0, 0, TILE, len(blocks)), (0, TILE, top - TILE, 0), *whole[1:]]


def thirds_of(rows):
    tiles = rows // TILE
    count = min(CUTS, tiles)
    cuts = [TILE * (tiles * i // count) for i in range(count + 1)]
    return [(a, b - a) for a, b in zip(cuts, cuts[1:])]


def rows_loop(first, rows, cols, body):
    step = TILE
    while rows % (2 * step) == 0 and 2 * step * cols <= 32 * 1024:
        step *= 2
    while rows % (3 * step) == 0 and 3 * step * cols <= 32 * 1024:
        step *= 3

    def one(i, carry):
        body(pl.ds(pl.multiple_of(first + i * step, TILE), step))
        return carry

    lax.fori_loop(0, rows // step, one, 0)


def kernel(n, *refs):
    g, w, m_in, v_in, w_out, m_out, v_out = (refs[i : i + 3] for i in range(0, 21, 3))
    own, term, run = (refs[i : i + 3] for i in range(21, 30, 3))
    stage, stage_sem, own_sem, own_short, mom_sem, term_recv, term_short, ring_recv, ring_send, chip_send, fw_recv, down_recv, down_send = refs[30:]
    chips = n // 2
    last = chips - 1
    me = lax.axis_index("dp")
    z, core = me // 2, lax.rem(me, 2)
    partner = me + 1 - 2 * core
    sign = (1, -1)
    ahead = [lax.rem(me + 2 * sign[d] + n, n) for d in range(2)]
    whole, head = pieces_of([one.shape[1:] for one in m_in])
    most, thirds = whole[:-1], thirds_of(whole[-1][2])

    def both(pieces):
        return [(p, d) for p in pieces for d in range(2)]

    def part(refs, p, *at):
        return refs[p[0]].at[(*at, pl.ds(p[1], p[2]))]

    def sem(many, short, p, d, slot):
        return short.at[d] if p[3] == len(whole) else many.at[d, slot, p[3]]

    def rs_block(d, s):
        return lax.rem(z - sign[d] * (s + 1) + 2 * chips, chips)

    def ag_block(d, t):
        return lax.rem(z - sign[d] * t + chips, chips)

    def remote(src, dst, send, recv, to):
        return pltpu.make_async_remote_copy(src_ref=src, dst_ref=dst, send_sem=send, recv_sem=recv, device_id={"dp": to}, device_id_type=MESH)

    def own_copy(p, d, s):
        slot = lax.rem(s, 2)
        return pltpu.make_async_copy(part(g, p, d, 2 * rs_block(d, s) + core), part(own, p, d, slot), sem(own_sem, own_short, p, d, slot))

    def stage_copy(p, d):
        return pltpu.make_async_copy(part(g, p, d, 2 * rs_block(d, 0) + 1 - core), stage.at[d], stage_sem.at[d])

    def term_copy(p, d, s, src=None):
        src = part(g, p, d, 2 * rs_block(d, s) + 1 - core) if src is None else src
        return remote(src, part(term, p, d, s), chip_send.at[p[0]], sem(term_recv, term_short, p, d, lax.rem(s, 2)), partner)

    def rs_copy(p, d, s):
        return remote(part(term, p, d, s), part(run, p, d, s), ring_send.at[p[0]], ring_recv.at[d, lax.rem(s, 3), p[0]], ahead[d])

    def ag_copy(p, d, t, block=None):
        at = part(w_out, p, d, 2 * (ag_block(d, t) if block is None else block) + core)
        return remote(at, at, ring_send.at[p[0]], ring_recv.at[d, lax.rem(last + t, 3), p[0]], ahead[d])

    def ag_arrival(p, d, t):
        return ag_copy(p, d, t, ag_block(d, t + 1))

    def fw_copy(p, d, t):
        at = part(w_out, p, d, 2 * ag_block(d, t) + core)
        return remote(at, at, chip_send.at[p[0]], fw_recv.at[p[0]], partner)

    def mom_copies(k):
        return (
            pltpu.make_async_copy(m_in[k], m_out[k], mom_sem.at[k]),
            pltpu.make_async_copy(v_in[k], v_out[k], mom_sem.at[k]),
            pltpu.make_async_copy(w[k].at[:, me], w_out[k].at[:, me], mom_sem.at[k]),
        )

    def bytes_of(at, semaphore):
        return pltpu.make_async_copy(at, at, semaphore)

    barrier = pltpu.get_barrier_semaphore()
    for peer in (partner, *ahead):
        pl.semaphore_signal(barrier, inc=1, device_id={"dp": peer}, device_id_type=MESH)
    for p, d in both(head[:1]):
        stage_copy(p, d).start()
    for p, d in both(head):
        own_copy(p, d, 0).start()
    pl.semaphore_wait(barrier, 3)

    for p, d in both(head):
        if p is head[0]:
            stage_copy(p, d).wait()
            term_copy(p, d, 0, stage.at[d]).start()
        else:
            term_copy(p, d, 0).start()

    def scatter_step(s, pieces, first):
        for p, d in both(pieces):
            k, row, rows, _ = p
            own_copy(p, d, s).wait()
            term_copy(p, d, s).wait_recv()
            if not first:
                rs_copy(p, d, s - 1).wait_recv()
            mine, other, sums = own[k].at[d, lax.rem(s, 2)], term[k].at[d, s], run[k].at[d, s - 1]

            def add(at):
                total = mine[at, :].astype(F32) + other[at, :].astype(F32)
                if not first:
                    total += sums[at, :].astype(F32)
                other[at, :] = total.astype(BF16)

            rows_loop(row, rows, mine.shape[1], add)
            if p[3] < len(whole):
                own_copy(whole[k], d, s + 1).start()
            rs_copy(p, d, s).start()
            if p[3] < len(whole):
                term_copy(whole[k], d, s + 1).start()

    scatter_step(0, head, True)
    for k in range(3):
        for copy in mom_copies(k):
            copy.start()
    lax.fori_loop(1, last, lambda s, c: (scatter_step(s, whole, False), c)[1], 0)

    for p, d in both(whole):
        k, row, rows, _ = p
        own_copy(p, d, last).wait()
        term_copy(p, d, last).wait_recv()
        if d == 0:
            bytes_of(w_out[k].at[0, pl.ds(0, 5 * m_in[k].shape[0])], mom_sem.at[k]).wait()
        rs_copy(p, d, last - 1).wait_recv()
        mine, other, sums = own[k].at[d, last % 2], term[k].at[d, last], run[k].at[d, last - 1]
        mo, vo, wo = m_out[k].at[d], v_out[k].at[d], w_out[k].at[d, me]

        def update(at):
            total = mine[at, :].astype(F32) + other[at, :].astype(F32) + sums[at, :].astype(F32)
            grad = total.astype(BF16).astype(F32)
            new_w, new_m, new_v = adamw(wo[at, :].astype(F32), mo[at, :], vo[at, :], grad)
            wo[at, :] = new_w
            mo[at, :] = new_m
            vo[at, :] = new_v

        rows_loop(row, rows, mine.shape[1], update)
        if p in most:
            ag_copy(p, d, 0).start()
            fw_copy(p, d, 0).start()

    def gather_step(t, c):
        for p, d in both(most):
            ag_arrival(p, d, t - 1).wait_recv()
            ag_copy(p, d, t).start()
            fw_copy(p, d, t).start()
        return c

    lax.fori_loop(1, last, gather_step, 0)
    def down_copy(p, d, t, block):
        at = w_out[-1].at[d, 2 * block + core, pl.ds(p[0], p[1])]
        return remote(at, at, down_send, down_recv.at[d, lax.rem(t, 3), thirds.index(p)], ahead[d])

    @pl.when(core == 1)
    def _():
        for p, d in both(thirds):
            down_copy(p, d, 0, ag_block(d, 0)).start()

    for p, d in both(most):
        ag_arrival(p, d, last - 1).wait_recv()
        fw_copy(p, d, last).start()

    @pl.when(core == 1)
    def _():
        def early_step(t, c):
            for p, d in both(thirds):
                down_copy(p, d, t - 1, ag_block(d, t)).wait_recv()
                down_copy(p, d, t, ag_block(d, t)).start()
            return c

        lax.fori_loop(1, EARLY, early_step, 0)
        for p, d in both(thirds):
            down_copy(p, d, EARLY - 1, ag_block(d, EARLY)).wait_recv()
        bytes_of(w_out[-1].at[0, pl.ds(0, 2 * EARLY)], down_send).wait()

    for k in range(3):
        if k < 2:
            bytes_of(w_out[k].at[:, pl.ds(0, n - 2)], ring_send.at[k]).wait()
            bytes_of(w_out[k], chip_send.at[k]).wait()
            bytes_of(w_out[k].at[0], fw_recv.at[k]).wait()
        else:
            bytes_of(w_out[k].at[0, pl.ds(0, n - 2)], ring_send.at[k]).wait()
            bytes_of(w_out[k].at[0], chip_send.at[k]).wait()


def rest_kernel(n, held, after, rest, ready, ring_send, ring_recv, chip_send, chip_recv):
    chips = n // 2
    last = chips - 1
    me = lax.axis_index("dp")
    z, core = me // 2, lax.rem(me, 2)
    partner = me + 1 - 2 * core
    sign = (1, -1)
    ahead = [lax.rem(me + 2 * sign[d] + n, n) for d in range(2)]
    thirds = thirds_of(held.shape[2])
    pieces = [(p, d) for p in thirds for d in range(2)]
    had = core * EARLY
    join = jnp.where(core == 0, JOIN, EARLY + 1)

    barrier = pltpu.get_barrier_semaphore()
    for peer in ahead:
        pl.semaphore_signal(barrier, inc=1, device_id={"dp": peer}, device_id_type=MESH)

    @pl.when(core == 0)
    def _():
        pl.semaphore_signal(barrier, inc=1, device_id={"dp": partner}, device_id_type=MESH)

    pl.semaphore_wait(barrier, 2 + core)

    @pl.when(core == 1)
    def _():
        pl.semaphore_signal(ready, inc=1, device_id={"dp": partner}, device_id_type=MESH)

    def at(ref, p, d, t):
        return ref.at[d, 2 * lax.rem(z - sign[d] * t + chips, chips) + core, pl.ds(p[0], p[1])]

    def remote(src, dst, send, recv, to):
        return pltpu.make_async_remote_copy(src_ref=src, dst_ref=dst, send_sem=send, recv_sem=recv, device_id={"dp": to}, device_id_type=MESH)

    def ring_copy(src, p, d, t):
        return remote(at(src, p, d, t), at(rest, p, d, t), ring_send, ring_recv.at[d, lax.rem(t, 3), thirds.index(p)], ahead[d])

    def arrive(p, d, t):
        there = at(rest, p, d, t)
        remote(there, there, ring_send, ring_recv.at[d, lax.rem(t - 1, 3), thirds.index(p)], ahead[d]).wait_recv()

    def fw_copy(src, p, d, t):
        return remote(at(src, p, d, t), at(rest, p, d, t), chip_send, chip_recv, partner)

    for p, d in pieces:
        ring_copy(held, p, d, had).start()

    def step(t, c, forward):
        for p, d in pieces:
            arrive(p, d, t)
            ring_copy(rest, p, d, t).start()
            if forward:
                fw_copy(rest, p, d, t).start()
        return c

    def catch_up(src):
        def one(t, c):
            for d in range(2):
                fw_copy(src, (0, held.shape[2]), d, t).start()
            return c

        return one

    lax.fori_loop(had + 1, join, functools.partial(step, forward=False), 0)

    @pl.when(core == 0)
    def _():
        pl.semaphore_wait(ready, 1)

    lax.fori_loop(0, had + 1, catch_up(held), 0)
    lax.fori_loop(had + 1, join, catch_up(rest), 0)
    lax.fori_loop(join, last, functools.partial(step, forward=True), 0)
    for p, d in pieces:
        arrive(p, d, last)
        fw_copy(rest, p, d, last).start()

    for which, count in enumerate((2 * last, 2 * (last - EARLY))):

        @pl.when(core == which)
        def _():
            part = rest.at[0, pl.ds(0, count)]
            pltpu.make_async_copy(part, part, ring_send).wait()

    pltpu.make_async_copy(rest.at[0], rest.at[0], chip_send).wait()
    pltpu.make_async_copy(rest.at[0], rest.at[0], chip_recv).wait()


def write_rest(n, held, rest, out, sem):
    chips = n // 2
    me = lax.axis_index("dp")
    z, core = me // 2, lax.rem(me, 2)
    for d, sign in ((0, 1), (1, -1)):
        for t in range(chips):
            block = 2 * lax.rem(z - sign * t + chips, chips) + core
            in_held = t <= core * EARLY
            for src, cond in ((held, in_held), (rest, jnp.logical_not(in_held))):

                @pl.when(cond)
                def _():
                    pltpu.make_async_copy(src.at[d, block], out.at[d, block], sem).start()

            other = 2 * t + 1 - core
            pltpu.make_async_copy(rest.at[d, other], out.at[d, other], sem).start()
    pltpu.make_async_copy(rest, rest, sem).wait()


def write_out(*refs):
    count = len(refs) // 2 - 1
    mark, sem = refs[-2:]
    copies = []
    for i in range(count):
        for j in range(refs[i].shape[0]):
            copies.append(pltpu.make_async_copy(refs[i].at[j], refs[count + i].at[j], sem.at[i, j]))
    for copy in copies:
        copy.start()
    mark[...] = jnp.zeros_like(mark)
    for copy in copies:
        copy.wait()


def solution(mesh):
    n = mesh.shape["dp"]
    chips = n // 2

    def step(*arrays):
        terms, weights, m, v = (arrays[i : i + 3] for i in (0, 3, 6, 9))
        layers = m[0].shape[0]
        blocks = [(one.shape[1], one.shape[2]) for one in m]
        terms = [t.reshape(layers, n, *b) for t, b in zip(terms, blocks, strict=True)]
        weights = [w.reshape(layers, n, *b) for w, b in zip(weights, blocks, strict=True)]
        dma = pltpu.SemaphoreType.DMA
        thirds = thirds_of(blocks[-1][0])
        out = pl.pallas_call(
            functools.partial(kernel, n),
            out_shape=[pltpu.VMEM((layers, n, *b), BF16) for b in blocks] + [pltpu.VMEM((layers, *b), F32) for b in blocks] * 2,
            in_specs=[pl.BlockSpec(memory_space=pltpu.HBM)] * 12,
            out_specs=[pl.BlockSpec(memory_space=pltpu.VMEM)] * 9,
            scratch_shapes=[
                *(pltpu.VMEM((layers, 2, *b), BF16) for b in blocks),
                *(pltpu.VMEM((layers, chips, *b), BF16) for b in blocks),
                *(pltpu.VMEM((layers, chips - 1, *b), BF16) for b in blocks),
                pltpu.VMEM((layers, TILE, blocks[0][1]), BF16),
                dma((layers,)),
                dma((layers, 2, 3)),
                dma((layers,)),
                dma((3,)),
                dma((layers, 2, 3)),
                dma((layers,)),
                dma((layers, 3, 3)),
                dma((3,)),
                dma((3,)),
                dma((3,)),
                dma((layers, 3, len(thirds))),
                dma,
            ],
            compiler_params=pltpu.CompilerParams(collective_id=0, has_side_effects=True, vmem_limit_bytes=28 * 1024 * 1024),
        )(*terms, *weights, *m, *v)
        held, ready = out[2], [*out[:2], *out[3:]]
        *done, mark = pl.pallas_call(
            write_out,
            out_shape=[*(pltpu.HBM(o.shape, o.dtype) for o in ready), jax.ShapeDtypeStruct((TILE, 128), F32)],
            in_specs=[pl.BlockSpec(memory_space=pltpu.VMEM)] * len(ready),
            out_specs=[pl.BlockSpec(memory_space=pltpu.HBM)] * len(ready) + [pl.BlockSpec(memory_space=pltpu.VMEM)],
            scratch_shapes=[dma((len(ready), layers))],
            compiler_params=pltpu.CompilerParams(vmem_limit_bytes=1024 * 1024),
        )(*ready)
        rest = pl.pallas_call(
            functools.partial(rest_kernel, n),
            out_shape=pltpu.VMEM(held.shape, held.dtype),
            in_specs=[pl.BlockSpec(memory_space=pltpu.VMEM)] * 2,
            out_specs=pl.BlockSpec(memory_space=pltpu.VMEM),
            scratch_shapes=[pltpu.SemaphoreType.REGULAR, dma, dma((layers, 3, len(thirds))), dma, dma],
            compiler_params=pltpu.CompilerParams(collective_id=1, has_side_effects=True, vmem_limit_bytes=1024 * 1024),
        )(held, mark)
        down = pl.pallas_call(
            functools.partial(write_rest, n),
            out_shape=pltpu.HBM(held.shape, held.dtype),
            in_specs=[pl.BlockSpec(memory_space=pltpu.VMEM)] * 2,
            out_specs=pl.BlockSpec(memory_space=pltpu.HBM),
            scratch_shapes=[dma],
            compiler_params=pltpu.CompilerParams(vmem_limit_bytes=1024 * 1024),
        )(held, rest)
        out = [*done[:2], down, *done[2:]]
        whole = [one.reshape(layers, n * b[0], b[1]) for one, b in zip(out[:3], blocks, strict=True)]
        return (*whole, *out[3:])

    all_of, cut = P(None, None, None), P(None, "dp", None)
    return jax.shard_map(
        step,
        mesh=mesh,
        in_specs=(P(("rep", "dp"), None, None, None),) * 3 + (all_of,) * 3 + (cut,) * 6,
        out_specs=(P("rep", None, None),) * 3 + (P("rep", "dp", None),) * 6,
        check_vma=False,
    )
```

```python
import functools

import jax
import jax.numpy as jnp
from jax import lax
from jax.experimental import pallas as pl
from jax.experimental.pallas import tpu as pltpu
from jax.sharding import PartitionSpec as P

MESH = pl.DeviceIdType.MESH
F32 = jnp.float32
BF16 = jnp.bfloat16
TILE = 8
EARLY = 6
JOIN = 6
CUTS = 9
CUTS_EARLY = 3


def adamw(w, m, v, g):
    m = 0.9 * m + 0.1 * g
    v = 0.95 * v + 0.05 * g * g
    step = m * lax.rsqrt(v + 1e-8) + 0.1 * w
    return (w - 0.02 * step).astype(BF16), m, v


def pieces_of(blocks):
    whole = [(k, 0, b[0], k) for k, b in enumerate(blocks)]
    top = blocks[0][0]
    return whole, [(0, 0, TILE, len(blocks)), (0, TILE, top - TILE, 0), *whole[1:]]


def thirds_of(rows, cuts=None):
    tiles = rows // TILE
    count = min(cuts or CUTS, tiles)
    cuts = [TILE * (tiles * i // count) for i in range(count + 1)]
    return [(a, b - a) for a, b in zip(cuts, cuts[1:])]


def rows_loop(first, rows, cols, body):
    step = TILE
    while rows % (2 * step) == 0 and 2 * step * cols <= 32 * 1024:
        step *= 2
    while rows % (3 * step) == 0 and 3 * step * cols <= 32 * 1024:
        step *= 3

    def one(i, carry):
        body(pl.ds(pl.multiple_of(first + i * step, TILE), step))
        return carry

    lax.fori_loop(0, rows // step, one, 0)


def kernel(n, *refs):
    g, w, m_in, v_in, w_out, m_out, v_out = (refs[i : i + 3] for i in range(0, 21, 3))
    own, term, run = (refs[i : i + 3] for i in range(21, 30, 3))
    stage, stage_sem, own_sem, own_short, mom_sem, term_recv, term_short, ring_recv, ring_send, chip_send, fw_recv, down_recv, down_send = refs[30:]
    chips = n // 2
    last = chips - 1
    me = lax.axis_index("dp")
    z, core = me // 2, lax.rem(me, 2)
    partner = me + 1 - 2 * core
    sign = (1, -1)
    ahead = [lax.rem(me + 2 * sign[d] + n, n) for d in range(2)]
    whole, head = pieces_of([one.shape[1:] for one in m_in])
    most, thirds = whole[:-1], thirds_of(whole[-1][2], CUTS_EARLY)

    def both(pieces):
        return [(p, d) for p in pieces for d in range(2)]

    def part(refs, p, *at):
        return refs[p[0]].at[(*at, pl.ds(p[1], p[2]))]

    def sem(many, short, p, d, slot):
        return short.at[d] if p[3] == len(whole) else many.at[d, slot, p[3]]

    def rs_block(d, s):
        return lax.rem(z - sign[d] * (s + 1) + 2 * chips, chips)

    def ag_block(d, t):
        return lax.rem(z - sign[d] * t + chips, chips)

    def remote(src, dst, send, recv, to):
        return pltpu.make_async_remote_copy(src_ref=src, dst_ref=dst, send_sem=send, recv_sem=recv, device_id={"dp": to}, device_id_type=MESH)

    def own_copy(p, d, s):
        slot = lax.rem(s, 2)
        return pltpu.make_async_copy(part(g, p, d, 2 * rs_block(d, s) + core), part(own, p, d, slot), sem(own_sem, own_short, p, d, slot))

    def stage_copy(p, d):
        return pltpu.make_async_copy(part(g, p, d, 2 * rs_block(d, 0) + 1 - core), stage.at[d], stage_sem.at[d])

    def term_copy(p, d, s, src=None):
        src = part(g, p, d, 2 * rs_block(d, s) + 1 - core) if src is None else src
        return remote(src, part(term, p, d, s), chip_send.at[p[0]], sem(term_recv, term_short, p, d, lax.rem(s, 2)), partner)

    def rs_copy(p, d, s):
        return remote(part(term, p, d, s), part(run, p, d, s), ring_send.at[p[0]], ring_recv.at[d, lax.rem(s, 3), p[0]], ahead[d])

    def ag_copy(p, d, t, block=None):
        at = part(w_out, p, d, 2 * (ag_block(d, t) if block is None else block) + core)
        return remote(at, at, ring_send.at[p[0]], ring_recv.at[d, lax.rem(last + t, 3), p[0]], ahead[d])

    def ag_arrival(p, d, t):
        return ag_copy(p, d, t, ag_block(d, t + 1))

    def fw_copy(p, d, t):
        at = part(w_out, p, d, 2 * ag_block(d, t) + core)
        return remote(at, at, chip_send.at[p[0]], fw_recv.at[p[0]], partner)

    def mom_copies(k):
        return (
            pltpu.make_async_copy(m_in[k], m_out[k], mom_sem.at[k]),
            pltpu.make_async_copy(v_in[k], v_out[k], mom_sem.at[k]),
            pltpu.make_async_copy(w[k].at[:, me], w_out[k].at[:, me], mom_sem.at[k]),
        )

    def bytes_of(at, semaphore):
        return pltpu.make_async_copy(at, at, semaphore)

    barrier = pltpu.get_barrier_semaphore()
    for peer in (partner, *ahead):
        pl.semaphore_signal(barrier, inc=1, device_id={"dp": peer}, device_id_type=MESH)
    for p, d in both(head[:1]):
        stage_copy(p, d).start()
    for p, d in both(head):
        own_copy(p, d, 0).start()
    pl.semaphore_wait(barrier, 3)

    for p, d in both(head):
        if p is head[0]:
            stage_copy(p, d).wait()
            term_copy(p, d, 0, stage.at[d]).start()
        else:
            term_copy(p, d, 0).start()

    def scatter_step(s, pieces, first):
        for p, d in both(pieces):
            k, row, rows, _ = p
            own_copy(p, d, s).wait()
            term_copy(p, d, s).wait_recv()
            if not first:
                rs_copy(p, d, s - 1).wait_recv()
            mine, other, sums = own[k].at[d, lax.rem(s, 2)], term[k].at[d, s], run[k].at[d, s - 1]

            def add(at):
                total = mine[at, :].astype(F32) + other[at, :].astype(F32)
                if not first:
                    total += sums[at, :].astype(F32)
                other[at, :] = total.astype(BF16)

            rows_loop(row, rows, mine.shape[1], add)
            if p[3] < len(whole):
                own_copy(whole[k], d, s + 1).start()
            rs_copy(p, d, s).start()
            if p[3] < len(whole):
                term_copy(whole[k], d, s + 1).start()

    scatter_step(0, head, True)
    for k in range(3):
        for copy in mom_copies(k):
            copy.start()
    lax.fori_loop(1, last, lambda s, c: (scatter_step(s, whole, False), c)[1], 0)

    for p, d in both(whole):
        k, row, rows, _ = p
        own_copy(p, d, last).wait()
        term_copy(p, d, last).wait_recv()
        if d == 0:
            bytes_of(w_out[k].at[0, pl.ds(0, 5 * m_in[k].shape[0])], mom_sem.at[k]).wait()
        rs_copy(p, d, last - 1).wait_recv()
        mine, other, sums = own[k].at[d, last % 2], term[k].at[d, last], run[k].at[d, last - 1]
        mo, vo, wo = m_out[k].at[d], v_out[k].at[d], w_out[k].at[d, me]

        def update(at):
            total = mine[at, :].astype(F32) + other[at, :].astype(F32) + sums[at, :].astype(F32)
            grad = total.astype(BF16).astype(F32)
            new_w, new_m, new_v = adamw(wo[at, :].astype(F32), mo[at, :], vo[at, :], grad)
            wo[at, :] = new_w
            mo[at, :] = new_m
            vo[at, :] = new_v

        rows_loop(row, rows, mine.shape[1], update)
        if p in most:
            ag_copy(p, d, 0).start()
            fw_copy(p, d, 0).start()

    def gather_step(t, c):
        for p, d in both(most):
            ag_arrival(p, d, t - 1).wait_recv()
            ag_copy(p, d, t).start()
            fw_copy(p, d, t).start()
        return c

    lax.fori_loop(1, last, gather_step, 0)
    def down_copy(p, d, t, block):
        at = w_out[-1].at[d, 2 * block + core, pl.ds(p[0], p[1])]
        return remote(at, at, down_send, down_recv.at[d, lax.rem(t, 3), thirds.index(p)], ahead[d])

    @pl.when(core == 1)
    def _():
        for p, d in both(thirds):
            down_copy(p, d, 0, ag_block(d, 0)).start()

    for p, d in both(most):
        ag_arrival(p, d, last - 1).wait_recv()
        fw_copy(p, d, last).start()

    @pl.when(core == 1)
    def _():
        def early_step(t, c):
            for p, d in both(thirds):
                down_copy(p, d, t - 1, ag_block(d, t)).wait_recv()
                down_copy(p, d, t, ag_block(d, t)).start()
            return c

        lax.fori_loop(1, EARLY, early_step, 0)
        for p, d in both(thirds):
            down_copy(p, d, EARLY - 1, ag_block(d, EARLY)).wait_recv()
        bytes_of(w_out[-1].at[0, pl.ds(0, 2 * EARLY)], down_send).wait()

    for k in range(3):
        if k < 2:
            bytes_of(w_out[k].at[:, pl.ds(0, n - 2)], ring_send.at[k]).wait()
            bytes_of(w_out[k], chip_send.at[k]).wait()
            bytes_of(w_out[k].at[0], fw_recv.at[k]).wait()
        else:
            bytes_of(w_out[k].at[0, pl.ds(0, n - 2)], ring_send.at[k]).wait()
            bytes_of(w_out[k].at[0], chip_send.at[k]).wait()


def rest_kernel(n, held, after, rest, ready, ring_send, ring_recv, chip_send, chip_recv):
    chips = n // 2
    last = chips - 1
    me = lax.axis_index("dp")
    z, core = me // 2, lax.rem(me, 2)
    partner = me + 1 - 2 * core
    sign = (1, -1)
    ahead = [lax.rem(me + 2 * sign[d] + n, n) for d in range(2)]
    thirds = thirds_of(held.shape[2])
    pieces = [(p, d) for p in thirds for d in range(2)]
    had = core * EARLY
    join = jnp.where(core == 0, JOIN, EARLY + 1)

    barrier = pltpu.get_barrier_semaphore()
    for peer in ahead:
        pl.semaphore_signal(barrier, inc=1, device_id={"dp": peer}, device_id_type=MESH)

    @pl.when(core == 0)
    def _():
        pl.semaphore_signal(barrier, inc=1, device_id={"dp": partner}, device_id_type=MESH)

    pl.semaphore_wait(barrier, 2 + core)

    @pl.when(core == 1)
    def _():
        pl.semaphore_signal(ready, inc=1, device_id={"dp": partner}, device_id_type=MESH)

    def at(ref, p, d, t):
        return ref.at[d, 2 * lax.rem(z - sign[d] * t + chips, chips) + core, pl.ds(p[0], p[1])]

    def remote(src, dst, send, recv, to):
        return pltpu.make_async_remote_copy(src_ref=src, dst_ref=dst, send_sem=send, recv_sem=recv, device_id={"dp": to}, device_id_type=MESH)

    def ring_copy(src, p, d, t):
        return remote(at(src, p, d, t), at(rest, p, d, t), ring_send, ring_recv.at[d, lax.rem(t, 3), thirds.index(p)], ahead[d])

    def arrive(p, d, t):
        there = at(rest, p, d, t)
        remote(there, there, ring_send, ring_recv.at[d, lax.rem(t - 1, 3), thirds.index(p)], ahead[d]).wait_recv()

    def fw_copy(src, p, d, t):
        return remote(at(src, p, d, t), at(rest, p, d, t), chip_send, chip_recv, partner)

    for p, d in pieces:
        ring_copy(held, p, d, had).start()

    def step(t, c, forward):
        for p, d in pieces:
            arrive(p, d, t)
            ring_copy(rest, p, d, t).start()
            if forward:
                fw_copy(rest, p, d, t).start()
        return c

    def catch_up(src):
        def one(t, c):
            for d in range(2):
                fw_copy(src, (0, held.shape[2]), d, t).start()
            return c

        return one

    lax.fori_loop(had + 1, join, functools.partial(step, forward=False), 0)

    @pl.when(core == 0)
    def _():
        pl.semaphore_wait(ready, 1)

    lax.fori_loop(0, had + 1, catch_up(held), 0)
    lax.fori_loop(had + 1, join, catch_up(rest), 0)
    lax.fori_loop(join, last, functools.partial(step, forward=True), 0)
    for p, d in pieces:
        arrive(p, d, last)
        fw_copy(rest, p, d, last).start()

    for which, count in enumerate((2 * last, 2 * (last - EARLY))):

        @pl.when(core == which)
        def _():
            part = rest.at[0, pl.ds(0, count)]
            pltpu.make_async_copy(part, part, ring_send).wait()

    pltpu.make_async_copy(rest.at[0], rest.at[0], chip_send).wait()
    pltpu.make_async_copy(rest.at[0], rest.at[0], chip_recv).wait()


def write_rest(n, held, rest, out, sem):
    chips = n // 2
    me = lax.axis_index("dp")
    z, core = me // 2, lax.rem(me, 2)
    for d, sign in ((0, 1), (1, -1)):
        for t in range(chips):
            block = 2 * lax.rem(z - sign * t + chips, chips) + core
            in_held = t <= core * EARLY
            for src, cond in ((held, in_held), (rest, jnp.logical_not(in_held))):

                @pl.when(cond)
                def _():
                    pltpu.make_async_copy(src.at[d, block], out.at[d, block], sem).start()

            other = 2 * t + 1 - core
            pltpu.make_async_copy(rest.at[d, other], out.at[d, other], sem).start()
    pltpu.make_async_copy(rest, rest, sem).wait()


def write_out(*refs):
    count = len(refs) // 2 - 1
    mark, sem = refs[-2:]
    copies = []
    for i in range(count):
        for j in range(refs[i].shape[0]):
            copies.append(pltpu.make_async_copy(refs[i].at[j], refs[count + i].at[j], sem.at[i, j]))
    for copy in copies:
        copy.start()
    mark[...] = jnp.zeros_like(mark)
    for copy in copies:
        copy.wait()


def solution(mesh):
    n = mesh.shape["dp"]
    chips = n // 2

    def step(*arrays):
        terms, weights, m, v = (arrays[i : i + 3] for i in (0, 3, 6, 9))
        layers = m[0].shape[0]
        blocks = [(one.shape[1], one.shape[2]) for one in m]
        terms = [t.reshape(layers, n, *b) for t, b in zip(terms, blocks, strict=True)]
        weights = [w.reshape(layers, n, *b) for w, b in zip(weights, blocks, strict=True)]
        dma = pltpu.SemaphoreType.DMA
        early, thirds = (thirds_of(blocks[-1][0], cuts) for cuts in (CUTS_EARLY, CUTS))
        out = pl.pallas_call(
            functools.partial(kernel, n),
            out_shape=[pltpu.VMEM((layers, n, *b), BF16) for b in blocks] + [pltpu.VMEM((layers, *b), F32) for b in blocks] * 2,
            in_specs=[pl.BlockSpec(memory_space=pltpu.HBM)] * 12,
            out_specs=[pl.BlockSpec(memory_space=pltpu.VMEM)] * 9,
            scratch_shapes=[
                *(pltpu.VMEM((layers, 2, *b), BF16) for b in blocks),
                *(pltpu.VMEM((layers, chips, *b), BF16) for b in blocks),
                *(pltpu.VMEM((layers, chips - 1, *b), BF16) for b in blocks),
                pltpu.VMEM((layers, TILE, blocks[0][1]), BF16),
                dma((layers,)),
                dma((layers, 2, 3)),
                dma((layers,)),
                dma((3,)),
                dma((layers, 2, 3)),
                dma((layers,)),
                dma((layers, 3, 3)),
                dma((3,)),
                dma((3,)),
                dma((3,)),
                dma((layers, 3, len(early))),
                dma,
            ],
            compiler_params=pltpu.CompilerParams(collective_id=0, has_side_effects=True, vmem_limit_bytes=28 * 1024 * 1024),
        )(*terms, *weights, *m, *v)
        held, ready = out[2], [*out[:2], *out[3:]]
        *done, mark = pl.pallas_call(
            write_out,
            out_shape=[*(pltpu.HBM(o.shape, o.dtype) for o in ready), jax.ShapeDtypeStruct((TILE, 128), F32)],
            in_specs=[pl.BlockSpec(memory_space=pltpu.VMEM)] * len(ready),
            out_specs=[pl.BlockSpec(memory_space=pltpu.HBM)] * len(ready) + [pl.BlockSpec(memory_space=pltpu.VMEM)],
            scratch_shapes=[dma((len(ready), layers))],
            compiler_params=pltpu.CompilerParams(vmem_limit_bytes=1024 * 1024),
        )(*ready)
        rest = pl.pallas_call(
            functools.partial(rest_kernel, n),
            out_shape=pltpu.VMEM(held.shape, held.dtype),
            in_specs=[pl.BlockSpec(memory_space=pltpu.VMEM)] * 2,
            out_specs=pl.BlockSpec(memory_space=pltpu.VMEM),
            scratch_shapes=[pltpu.SemaphoreType.REGULAR, dma, dma((layers, 3, len(thirds))), dma, dma],
            compiler_params=pltpu.CompilerParams(collective_id=1, has_side_effects=True, vmem_limit_bytes=1024 * 1024),
        )(held, mark)
        down = pl.pallas_call(
            functools.partial(write_rest, n),
            out_shape=pltpu.HBM(held.shape, held.dtype),
            in_specs=[pl.BlockSpec(memory_space=pltpu.VMEM)] * 2,
            out_specs=pl.BlockSpec(memory_space=pltpu.HBM),
            scratch_shapes=[dma],
            compiler_params=pltpu.CompilerParams(vmem_limit_bytes=1024 * 1024),
        )(held, rest)
        out = [*done[:2], down, *done[2:]]
        whole = [one.reshape(layers, n * b[0], b[1]) for one, b in zip(out[:3], blocks, strict=True)]
        return (*whole, *out[3:])

    all_of, cut = P(None, None, None), P(None, "dp", None)
    return jax.shard_map(
        step,
        mesh=mesh,
        in_specs=(P(("rep", "dp"), None, None, None),) * 3 + (all_of,) * 3 + (cut,) * 6,
        out_specs=(P("rep", None, None),) * 3 + (P("rep", "dp", None),) * 6,
        check_vma=False,
    )
```
